256 devices in a mesh: ctx: 64 (over z, x, core), heads: 4 (over y).
Axes of the slice: x: 4, y: 4, z: 8, core: 2. Of those that a mesh axis runs over, the one named last changes fastest.
Arguments:
- query_rows: bfloat16 [64, 16, 2, 128], P('ctx', 'heads'), may hold values from -6 to 6
- past_keys: bfloat16 [64, 16, 4096, 128], P(None, 'heads', 'ctx'), may hold values from -6 to 6
- past_values: bfloat16 [64, 16, 4096, 128], P(None, 'heads', 'ctx'), may hold values from -6 to 6
- used_length: int32 [64], replicated, may hold values from 2048 to 4096
Outputs:
- read: bfloat16 [64, 16, 2, 128], P('ctx', 'heads')
The draws below stay inside these ranges and needn't reach their ends.
All inputs are finite; a program needn't handle non-finite values.
Results may differ from the reference program's by a relative error of at most 0.0015.
Values may be sent and summed in bfloat16 or wider, within the bound.
A program may use at most 64 MiB of HBM per device.

```python
import jax
import jax.numpy as jnp
from jax import lax

BATCH = 64
LENGTH = 4096
KV_HEADS = 16
GROUP = 2
HEAD_SIZE = 128


def set_ends(result, key, least, largest):
    place = [jax.random.randint(jax.random.fold_in(key, axis), (), 0, length) for axis, length in enumerate(result.shape)]
    main_axis = result.shape.index(max(result.shape))
    beside = place[:main_axis] + [(place[main_axis] + 1) % result.shape[main_axis]] + place[main_axis + 1:]
    return result.at[tuple(place)].set(least).at[tuple(beside)].set(largest)


def shard_levels(stream_key, extent, pieces, least, largest):
    def one(position, shards_of):
        draws = jax.random.uniform(jax.random.fold_in(jax.random.fold_in(stream_key, 6), position), (shards_of,), jnp.float32, least / len(pieces), largest / len(pieces))
        return jnp.repeat(jnp.exp(draws), extent[position] // shards_of).reshape((-1,) + (1,) * (len(extent) - position - 1))

    factor_of = one(*pieces[0])
    for cut in pieces[1:]:
        factor_of = factor_of * one(*cut)
    return factor_of


def gaussian(rng, shape, width, most, cuts=(), kind=jnp.bfloat16):
    drawn = width * jax.random.normal(rng, shape, jnp.float32)
    if cuts:
        drawn = drawn * shard_levels(rng, shape, cuts, -0.22, 0.18)
    return jnp.clip(drawn, -most, most).astype(kind)


def setup_inputs(seed: int = 0) -> dict:
    key_of = jax.random.split(jax.random.key(seed), 5)
    query_rows = gaussian(key_of[0], (BATCH, KV_HEADS, GROUP, HEAD_SIZE), 1.0, 6.0, ((0, 64), (1, 4)))
    past_keys = gaussian(key_of[1], (BATCH, KV_HEADS, LENGTH, HEAD_SIZE), 1.0, 6.0, ((1, 4), (2, 64)))
    past_values = gaussian(key_of[2], (BATCH, KV_HEADS, LENGTH, HEAD_SIZE), 1.0, 6.0, ((1, 4), (2, 64)))
    used_length = set_ends(jax.random.randint(key_of[3], (BATCH,), LENGTH // 2, LENGTH + 1), jax.random.fold_in(key_of[3], 1), LENGTH // 2, LENGTH).astype(jnp.int32)
    return dict(query_rows=query_rows, past_keys=past_keys, past_values=past_values, used_length=used_length)


def reference(query_rows, past_keys, past_values, used_length):
    def one_sequence(item):
        query_one, keys_one, values_one, length_one = item
        logit = jnp.einsum("kgd,ktd->kgt", query_one.astype(jnp.float32), keys_one.astype(jnp.float32)) * HEAD_SIZE ** -0.5
        logit = jnp.where(jnp.arange(LENGTH) < length_one, logit, -1e30)
        share = jax.nn.softmax(logit, axis=-1)
        return jnp.einsum("kgt,ktd->kgd", share, values_one.astype(jnp.float32), precision=lax.Precision.HIGHEST)
    read = lax.map(one_sequence, (query_rows, past_keys, past_values, used_length)).astype(jnp.bfloat16)
    return read
```

```python
import jax
import jax.numpy as jnp
from jax import lax
from jax.experimental import pallas as pl
from jax.experimental.pallas import tpu as pltpu
from jax.sharding import PartitionSpec as P

MESH = pl.DeviceIdType.MESH
ZS, XS, CS = 8, 4, 2
STRETCHES = ZS * XS * CS
HEADS, GROUP, STRETCH, SIZE = 4, 2, 64, 128
ROWS, COLS = HEADS * GROUP, HEADS * STRETCH
MASKED = -1e30
BESIDE = [(x, c) for x in (0, 1, 3, 2) for c in range(CS)]


def ring_place(i):
    return lax.rem(jnp.where(lax.rem(i, 2) == 1, (i + 1) // 2, ZS - i // 2), ZS)


def ring_order(i):
    return jnp.where(i == 0, 0, jnp.where(i == ZS - 1, ZS - 1, jnp.where(lax.rem(i, 2) == 1, i + 1, i - 1)))


def kernel(query, keys, values, lengths, out, k_buf, v_buf, q_buf, len_buf, part, parts, q_send, q_recv, p_send, p_recv, k_sem, v_sem, in_sem):
    me = lax.axis_index("ctx")
    my_z, my_x, my_c = me // (XS * CS), lax.rem(me // CS, XS), lax.rem(me, CS)

    def owner(i, x, c):
        z = lax.rem(my_z + ring_place(i), ZS)
        return (z * XS + lax.rem(my_x + x, XS)) * CS + lax.rem(my_c + c, CS)

    def others(do):
        for x, c in BESIDE[1:]:
            do(0, x, c)

        @pl.loop(1, ZS)
        def _(i):
            for x, c in BESIDE:
                do(i, x, c)

    barrier = pltpu.get_barrier_semaphore()

    def greet(i, x, c):
        pl.semaphore_signal(barrier, inc=1, device_id={"ctx": owner(i, x, c)}, device_id_type=MESH)

    others(greet)
    own_copy = pltpu.make_async_copy(query, q_buf.at[me], in_sem.at[0])
    own_copy.start()
    len_copy = pltpu.make_async_copy(lengths, len_buf, in_sem.at[1])
    len_copy.start()
    k_copy = pltpu.make_async_copy(keys, k_buf, k_sem)
    k_copy.start()
    v_copy = pltpu.make_async_copy(values, v_buf, v_sem)
    v_copy.start()
    own_copy.wait()
    len_copy.wait()
    pl.semaphore_wait(barrier, STRETCHES - 1)

    def ask(i, x, c):
        pltpu.make_async_remote_copy(
            src_ref=q_buf.at[me],
            dst_ref=q_buf.at[me],
            send_sem=q_send,
            recv_sem=q_recv.at[ring_order(i)],
            device_id={"ctx": owner(i, x, c)},
            device_id_type=MESH,
        ).start()

    others(ask)
    k_copy.wait()
    v_copy.wait()

    row = lax.broadcasted_iota(jnp.int32, (ROWS, COLS), 0)
    col = lax.broadcasted_iota(jnp.int32, (ROWS, COLS), 1)
    own_head = row // GROUP == col // STRETCH
    position = me * STRETCH + lax.rem(col, STRETCH)
    slot_row = lax.broadcasted_iota(jnp.int32, (ROWS, SIZE), 0)
    slot = lax.broadcasted_iota(jnp.int32, (ROWS, SIZE), 1)

    def partial(b):
        logit = lax.dot_general(
            q_buf[b], k_buf[b], (((1,), (1,)), ((), ())), preferred_element_type=jnp.float32
        ) * SIZE ** (-0.5)
        filled = own_head & (position < len_buf[b])
        logit = jnp.where(filled, logit, MASKED)
        top = jnp.max(logit, axis=1, keepdims=True)
        share = jnp.where(filled, jnp.exp(logit - top), 0.0)
        weight = jnp.sum(share, axis=1, keepdims=True)
        coarse = share.astype(jnp.bfloat16).astype(jnp.float32)
        halves = jnp.concatenate([coarse, share - coarse], axis=0).astype(jnp.bfloat16)
        read = jnp.dot(halves, v_buf[b], preferred_element_type=jnp.float32)
        stats = jnp.where(slot == slot_row, top, jnp.where(slot == slot_row + ROWS, weight, 0.0))
        return read[:ROWS] + read[ROWS:], jnp.sum(stats, axis=0, keepdims=True)

    def answer(i, x, c):
        b = owner(i, x, c)
        read, stats = partial(b)
        part[b, pl.ds(0, ROWS), :] = read
        part[b, pl.ds(ROWS, 1), :] = stats

    def give(i, x, c):
        b = owner(i, x, c)
        pltpu.make_async_remote_copy(
            src_ref=part.at[b],
            dst_ref=parts.at[me],
            send_sem=p_send,
            recv_sem=p_recv,
            device_id={"ctx": b},
            device_id_type=MESH,
        ).start()

    def arrived(n, i):
        pltpu.make_async_copy(q_buf.at[pl.ds(0, n)], q_buf.at[pl.ds(0, n)], q_recv.at[i]).wait()

    read, stats = partial(me)
    parts[me, pl.ds(0, ROWS), :] = read
    parts[me, pl.ds(ROWS, 1), :] = stats
    arrived(len(BESIDE) - 1, 0)
    for x, c in BESIDE[1:]:
        answer(0, x, c)
    for x, c in BESIDE[1:]:
        give(0, x, c)

    @pl.loop(1, ZS)
    def _(i):
        arrived(len(BESIDE), i)
        for x, c in BESIDE:
            answer(i, x, c)
        for x, c in BESIDE:
            give(i, x, c)

    rest = pl.ds(0, STRETCHES - 1)
    pltpu.make_async_copy(parts.at[rest], parts.at[rest], p_recv).wait()

    stats = parts[:, ROWS, :]
    scale = jnp.exp(stats - jnp.max(stats, axis=0, keepdims=True))
    weight = jnp.sum(scale * pltpu.roll(stats, SIZE - ROWS, 1), axis=0, keepdims=True)
    scale = jnp.transpose(scale / weight)[:ROWS, :]
    total = jnp.zeros((ROWS, SIZE), jnp.float32)
    for s in range(STRETCHES):
        total += scale[:, s : s + 1] * parts[s, pl.ds(0, ROWS), :]
    out[...] = total.astype(out.dtype)

    pltpu.make_async_copy(q_buf.at[rest], q_buf.at[rest], q_send).wait()
    pltpu.make_async_copy(part.at[rest], part.at[rest], p_send).wait()


def body(query_rows, past_keys, past_values, used_length):
    anywhere = pl.BlockSpec(memory_space=pl.ANY)
    read = pl.pallas_call(
        kernel,
        out_shape=jax.ShapeDtypeStruct((ROWS, SIZE), jnp.bfloat16),
        in_specs=[anywhere] * 4,
        out_specs=pl.BlockSpec(memory_space=pltpu.VMEM),
        scratch_shapes=[
            pltpu.VMEM((STRETCHES, COLS, SIZE), jnp.bfloat16),
            pltpu.VMEM((STRETCHES, COLS, SIZE), jnp.bfloat16),
            pltpu.VMEM((STRETCHES, ROWS, SIZE), jnp.bfloat16),
            pltpu.SMEM((STRETCHES,), jnp.int32),
            pltpu.VMEM((STRETCHES, ROWS + 1, SIZE), jnp.float32),
            pltpu.VMEM((STRETCHES, ROWS + 1, SIZE), jnp.float32),
            pltpu.SemaphoreType.DMA,
            pltpu.SemaphoreType.DMA((ZS,)),
            pltpu.SemaphoreType.DMA,
            pltpu.SemaphoreType.DMA,
            pltpu.SemaphoreType.DMA,
            pltpu.SemaphoreType.DMA,
            pltpu.SemaphoreType.DMA((2,)),
        ],
        compiler_params=pltpu.CompilerParams(collective_id=0, has_side_effects=True),
    )(
        query_rows.reshape(ROWS, SIZE),
        past_keys.reshape(STRETCHES, COLS, SIZE),
        past_values.reshape(STRETCHES, COLS, SIZE),
        used_length,
    )
    return read.reshape(query_rows.shape)


def solution(mesh):
    return jax.shard_map(
        body,
        mesh=mesh,
        in_specs=(
            P("ctx", "heads", None, None),
            P(None, "heads", "ctx", None),
            P(None, "heads", "ctx", None),
            P(),
        ),
        out_specs=P("ctx", "heads", None, None),
        check_vma=False,
    )
```

```python
import jax
import jax.numpy as jnp
from jax import lax
from jax.experimental import pallas as pl
from jax.experimental.pallas import tpu as pltpu
from jax.sharding import PartitionSpec as P

MESH = pl.DeviceIdType.MESH
ZS, XS, CS = 8, 4, 2
STRETCHES = ZS * XS * CS
HEADS, GROUP, STRETCH, SIZE = 4, 2, 64, 128
ROWS, COLS = HEADS * GROUP, HEADS * STRETCH
MASKED = -1e30
FAR = (4, 5, 3, 6, 2, 7, 1, 0)
BESIDE = [(x, c) for x in (2, 1, 3, 0) for c in (1, 0)]


def kernel(query, keys, values, lengths, out, k_buf, v_buf, q_buf, len_buf, part, parts, q_send, q_recv, p_send, p_recv, k_sem, v_sem, in_sem):
    me = lax.axis_index("ctx")
    my_z, my_x, my_c = me // (XS * CS), lax.rem(me // CS, XS), lax.rem(me, CS)

    def owner(z, x, c):
        return (z * XS + lax.rem(my_x + x, XS)) * CS + lax.rem(my_c + c, CS)

    def others(do):
        for step in FAR:
            z = lax.rem(my_z + step, ZS)
            for x, c in BESIDE:
                if (step, x, c) != (0, 0, 0):
                    do(owner(z, x, c))

    barrier = pltpu.get_barrier_semaphore()

    def greet(b):
        pl.semaphore_signal(barrier, inc=1, device_id={"ctx": b}, device_id_type=MESH)

    others(greet)
    own_copy = pltpu.make_async_copy(query, q_buf.at[me], in_sem.at[0])
    own_copy.start()
    len_copy = pltpu.make_async_copy(lengths, len_buf, in_sem.at[1])
    len_copy.start()
    k_copy = pltpu.make_async_copy(keys, k_buf, k_sem)
    k_copy.start()
    v_copy = pltpu.make_async_copy(values, v_buf, v_sem)
    v_copy.start()
    own_copy.wait()
    len_copy.wait()
    pl.semaphore_wait(barrier, STRETCHES - 1)

    def ask(b):
        pltpu.make_async_remote_copy(
            src_ref=q_buf.at[me],
            dst_ref=q_buf.at[me],
            send_sem=q_send,
            recv_sem=q_recv.at[my_z],
            device_id={"ctx": b},
            device_id_type=MESH,
        ).start()

    others(ask)
    k_copy.wait()
    v_copy.wait()

    row = lax.broadcasted_iota(jnp.int32, (ROWS, COLS), 0)
    col = lax.broadcasted_iota(jnp.int32, (ROWS, COLS), 1)
    own_head = row // GROUP == col // STRETCH
    position = me * STRETCH + lax.rem(col, STRETCH)
    slot_row = lax.broadcasted_iota(jnp.int32, (ROWS, SIZE), 0)
    slot = lax.broadcasted_iota(jnp.int32, (ROWS, SIZE), 1)

    def answer(owners):
        logits = [
            lax.dot_general(q_buf[b], k_buf[b], (((1,), (1,)), ((), ())), preferred_element_type=jnp.float32)
            for b in owners
        ]
        halves, tops, weights = [], [], []
        for b, logit in zip(owners, logits):
            filled = own_head & (position < len_buf[b])
            logit = jnp.where(filled, logit * SIZE ** (-0.5), MASKED)
            top = jnp.max(logit, axis=1, keepdims=True)
            share = jnp.where(filled, jnp.exp(logit - top), 0.0)
            coarse = share.astype(jnp.bfloat16).astype(jnp.float32)
            halves.append(jnp.concatenate([coarse, share - coarse], axis=0).astype(jnp.bfloat16))
            tops.append(top)
            weights.append(jnp.sum(share, axis=1, keepdims=True))
        reads = [jnp.dot(half, v_buf[b], preferred_element_type=jnp.float32) for b, half in zip(owners, halves)]
        for b, read, top, weight in zip(owners, reads, tops, weights):
            stats = jnp.where(slot == slot_row, top, jnp.where(slot == slot_row + ROWS, weight, 0.0))
            part[b, pl.ds(0, ROWS), :] = read[:ROWS] + read[ROWS:]
            part[b, pl.ds(ROWS, 1), :] = jnp.sum(stats, axis=0, keepdims=True)

    def give(b):
        @pl.when(b != me)
        def _():
            pltpu.make_async_remote_copy(
                src_ref=part.at[b],
                dst_ref=parts.at[me],
                send_sem=p_send,
                recv_sem=p_recv,
                device_id={"ctx": b},
                device_id_type=MESH,
            ).start()

    def arrived(z):
        def wait(n):
            pltpu.make_async_copy(q_buf.at[pl.ds(0, n)], q_buf.at[pl.ds(0, n)], q_recv.at[z]).wait()

        pl.when(z == my_z)(lambda: wait(len(BESIDE) - 1))
        pl.when(z != my_z)(lambda: wait(len(BESIDE)))

    @pl.loop(0, ZS)
    def _(z):
        arrived(z)
        owners = [owner(z, x, c) for x, c in BESIDE]
        answer(owners)
        for b in owners:
            give(b)

    parts[me] = part[me]
    rest = pl.ds(0, STRETCHES - 1)
    pltpu.make_async_copy(parts.at[rest], parts.at[rest], p_recv).wait()

    stats = parts[:, ROWS, :]
    scale = jnp.exp(stats - jnp.max(stats, axis=0, keepdims=True))
    weight = jnp.sum(scale * pltpu.roll(stats, SIZE - ROWS, 1), axis=0, keepdims=True)
    scale = jnp.transpose(scale / weight)[:ROWS, :]
    total = jnp.zeros((ROWS, SIZE), jnp.float32)
    for s in range(STRETCHES):
        total += scale[:, s : s + 1] * parts[s, pl.ds(0, ROWS), :]
    out[...] = total.astype(out.dtype)

    pltpu.make_async_copy(q_buf.at[rest], q_buf.at[rest], q_send).wait()
    pltpu.make_async_copy(part.at[rest], part.at[rest], p_send).wait()


def body(query_rows, past_keys, past_values, used_length):
    anywhere = pl.BlockSpec(memory_space=pl.ANY)
    read = pl.pallas_call(
        kernel,
        out_shape=jax.ShapeDtypeStruct((ROWS, SIZE), jnp.bfloat16),
        in_specs=[anywhere] * 4,
        out_specs=pl.BlockSpec(memory_space=pltpu.VMEM),
        scratch_shapes=[
            pltpu.VMEM((STRETCHES, COLS, SIZE), jnp.bfloat16),
            pltpu.VMEM((STRETCHES, COLS, SIZE), jnp.bfloat16),
            pltpu.VMEM((STRETCHES, ROWS, SIZE), jnp.bfloat16),
            pltpu.SMEM((STRETCHES,), jnp.int32),
            pltpu.VMEM((STRETCHES, ROWS + 1, SIZE), jnp.float32),
            pltpu.VMEM((STRETCHES, ROWS + 1, SIZE), jnp.float32),
            pltpu.SemaphoreType.DMA,
            pltpu.SemaphoreType.DMA((ZS,)),
            pltpu.SemaphoreType.DMA,
            pltpu.SemaphoreType.DMA,
            pltpu.SemaphoreType.DMA,
            pltpu.SemaphoreType.DMA,
            pltpu.SemaphoreType.DMA((2,)),
        ],
        compiler_params=pltpu.CompilerParams(collective_id=0, has_side_effects=True),
    )(
        query_rows.reshape(ROWS, SIZE),
        past_keys.reshape(STRETCHES, COLS, SIZE),
        past_values.reshape(STRETCHES, COLS, SIZE),
        used_length,
    )
    return read.reshape(query_rows.shape)


def solution(mesh):
    return jax.shard_map(
        body,
        mesh=mesh,
        in_specs=(
            P("ctx", "heads", None, None),
            P(None, "heads", "ctx", None),
            P(None, "heads", "ctx", None),
            P(),
        ),
        out_specs=P("ctx", "heads", None, None),
        check_vma=False,
    )
```

```python
import jax
import jax.numpy as jnp
from jax import lax
from jax.experimental import pallas as pl
from jax.experimental.pallas import tpu as pltpu
from jax.sharding import PartitionSpec as P

MESH = pl.DeviceIdType.MESH
ZS, XS, CS = 8, 4, 2
STRETCHES = ZS * XS * CS
HEADS, GROUP, STRETCH, SIZE = 4, 2, 64, 128
ROWS, COLS = HEADS * GROUP, HEADS * STRETCH
MASKED = -1e30
CHIPS = ZS * XS
FAR = (4, 5, 3, 6, 2, 7, 1, 0)
ACROSS = (2, 1, 3, 0)
EARLY = 2
NEAREST = [min(range(EARLY), key=lambda e: min((z - e) % ZS, (e - z) % ZS)) for z in range(ZS)]


def kernel(
    query, keys, values, lengths, out, k_buf, v_buf, q_buf, len_buf, part, parts,
    q_send, q_recv, p_send, p_recv, k_own, v_own, k_send, v_send, k_recv, v_recv, in_sem, there, all_there,
):
    me = lax.axis_index("ctx")
    my_z, my_x, my_c = me // (XS * CS), lax.rem(me // CS, XS), lax.rem(me, CS)
    chip, beside = me // CS, me + 1 - 2 * my_c
    first = my_z < EARLY

    def turn(k):
        return jnp.where(k < ZS // 2, k, ZS + ZS // 2 - 1 - k)

    def device(z, x):
        return (z * XS + x) * CS + my_c

    def in_plane(z, do):
        for across in ACROSS:
            x = lax.rem(my_x + across, XS)
            if across:
                do(device(z, x))
            else:
                pl.when(z != my_z)(lambda: do(device(z, x)))

    def beyond(do):
        for step in FAR:
            z = lax.rem(my_z + step, ZS)
            pl.when(z >= EARLY)(lambda: in_plane(z, do))

    def within(do):
        for z in range(EARLY):
            in_plane(z, do)

    barrier = pltpu.get_barrier_semaphore()

    def tell(sem, b):
        pl.semaphore_signal(sem, inc=1, device_id={"ctx": b}, device_id_type=MESH)

    def greet(b):
        tell(barrier, b)

    greet(beside)

    @pl.when(first)
    def _():
        beyond(greet)
        within(greet)

    own_copy = pltpu.make_async_copy(query, q_buf.at[chip], in_sem.at[0])
    own_copy.start()
    len_copy = pltpu.make_async_copy(lengths, len_buf, in_sem.at[1])
    len_copy.start()
    k_copy = pltpu.make_async_copy(keys.at[:, my_c], k_buf.at[:, my_c], k_own)
    k_copy.start()
    v_copy = pltpu.make_async_copy(values.at[:, my_c], v_buf.at[:, my_c], v_own)
    v_copy.start()
    pl.when(first)(lambda: pl.semaphore_wait(barrier, EARLY * XS))

    @pl.when(~first)
    def _():
        pl.semaphore_wait(barrier, EARLY * XS + 1)
        within(lambda b: tell(there, b))

    own_copy.wait()
    len_copy.wait()

    def ask(b):
        pltpu.make_async_remote_copy(
            src_ref=q_buf.at[chip],
            dst_ref=q_buf.at[chip],
            send_sem=q_send,
            recv_sem=q_recv.at[my_z],
            device_id={"ctx": b},
            device_id_type=MESH,
        ).start()

    within(ask)

    def swap(z, source, buffer, send_sem, recv_sem):
        rows = pl.ds(z * XS, XS)
        return pltpu.make_async_remote_copy(
            src_ref=source.at[rows, 1 - my_c],
            dst_ref=buffer.at[rows, my_c],
            send_sem=send_sem,
            recv_sem=recv_sem.at[z],
            device_id={"ctx": beside},
            device_id_type=MESH,
        )

    @pl.loop(0, ZS)
    def _(k):
        swap(turn(k), keys, k_buf, k_send, k_recv).start()
        swap(turn(k), values, v_buf, v_send, v_recv).start()

    def arrived(z):
        def wait(n):
            pltpu.make_async_copy(q_buf.at[pl.ds(0, n)], q_buf.at[pl.ds(0, n)], q_recv.at[z]).wait()

        pl.when(z == my_z)(lambda: wait(XS - 1))
        pl.when(z != my_z)(lambda: wait(XS))

    @pl.when(first)
    def _():
        pl.semaphore_wait(there, (ZS - EARLY) * XS)
        for z in range(EARLY, ZS):
            pl.when(my_z == NEAREST[z])(lambda z=z: tell(all_there, device(z, my_x)))

    pl.when(~first)(lambda: pl.semaphore_wait(all_there, 1))
    beyond(ask)
    k_copy.wait()
    v_copy.wait()

    row = lax.broadcasted_iota(jnp.int32, (ROWS, COLS), 0)
    col = lax.broadcasted_iota(jnp.int32, (ROWS, COLS), 1)
    own_head = row // GROUP == col // STRETCH
    position = [(chip * CS + c) * STRETCH + lax.rem(col, STRETCH) for c in range(CS)]
    slot_row = lax.broadcasted_iota(jnp.int32, (ROWS, SIZE), 0)
    slot = lax.broadcasted_iota(jnp.int32, (ROWS, SIZE), 1)

    def answer(z):
        owners = [z * XS + x for x in range(XS)]
        logits = [
            [
                lax.dot_general(q_buf[i], k_buf[i, c], (((1,), (1,)), ((), ())), preferred_element_type=jnp.float32)
                for c in range(CS)
            ]
            for i in owners
        ]
        halves, tops, weights = [], [], []
        for i, pair in zip(owners, logits):
            length = len_buf[i * CS + my_c]
            filled = [own_head & (position[c] < length) for c in range(CS)]
            pair = [jnp.where(f, logit * SIZE ** (-0.5), MASKED) for f, logit in zip(filled, pair)]
            top = jnp.max(jnp.maximum(*pair), axis=1, keepdims=True)
            shares = [jnp.where(f, jnp.exp(logit - top), 0.0) for f, logit in zip(filled, pair)]
            coarse = [share.astype(jnp.bfloat16).astype(jnp.float32) for share in shares]
            halves.append(
                [jnp.concatenate([c, share - c], axis=0).astype(jnp.bfloat16) for c, share in zip(coarse, shares)]
            )
            tops.append(top)
            weights.append(jnp.sum(shares[0] + shares[1], axis=1, keepdims=True))
        reads = [
            sum(jnp.dot(halves_of[c], v_buf[i, c], preferred_element_type=jnp.float32) for c in range(CS))
            for i, halves_of in zip(owners, halves)
        ]
        for i, read, top, weight in zip(owners, reads, tops, weights):
            stats = jnp.where(slot == slot_row, top, jnp.where(slot == slot_row + ROWS, weight, 0.0))
            part[i, pl.ds(0, ROWS), :] = read[:ROWS] + read[ROWS:]
            part[i, pl.ds(ROWS, 1), :] = jnp.sum(stats, axis=0, keepdims=True)

    def give(b):
        pltpu.make_async_remote_copy(
            src_ref=part.at[b // CS],
            dst_ref=parts.at[chip],
            send_sem=p_send,
            recv_sem=p_recv,
            device_id={"ctx": b},
            device_id_type=MESH,
        ).start()

    @pl.loop(0, ZS)
    def _(k):
        z = turn(k)
        arrived(z)
        swap(z, keys, k_buf, k_send, k_recv).wait_recv()
        swap(z, values, v_buf, v_send, v_recv).wait_recv()
        answer(z)
        in_plane(z, give)

    parts[chip] = part[chip]

    rest = pl.ds(0, CHIPS - 1)
    pltpu.make_async_copy(parts.at[rest], parts.at[rest], p_recv).wait()

    stats = parts[:, ROWS, :]
    scale = jnp.exp(stats - jnp.max(stats, axis=0, keepdims=True))
    weight = jnp.sum(scale * pltpu.roll(stats, SIZE - ROWS, 1), axis=0, keepdims=True)
    scale = jnp.transpose(scale / weight)[:ROWS, :]
    total = jnp.zeros((ROWS, SIZE), jnp.float32)
    for s in range(CHIPS):
        total += scale[:, s : s + 1] * parts[s, pl.ds(0, ROWS), :]
    out[...] = total.astype(out.dtype)

    pltpu.make_async_copy(q_buf.at[rest], q_buf.at[rest], q_send).wait()
    pltpu.make_async_copy(part.at[rest], part.at[rest], p_send).wait()
    pltpu.make_async_copy(k_buf.at[:, 0], k_buf.at[:, 0], k_send).wait()
    pltpu.make_async_copy(v_buf.at[:, 0], v_buf.at[:, 0], v_send).wait()


def body(query_rows, past_keys, past_values, used_length):
    anywhere = pl.BlockSpec(memory_space=pl.ANY)
    dma = pltpu.SemaphoreType.DMA
    read = pl.pallas_call(
        kernel,
        out_shape=jax.ShapeDtypeStruct((ROWS, SIZE), jnp.bfloat16),
        in_specs=[anywhere] * 4,
        out_specs=pl.BlockSpec(memory_space=pltpu.VMEM),
        scratch_shapes=[
            pltpu.VMEM((CHIPS, CS, COLS, SIZE), jnp.bfloat16),
            pltpu.VMEM((CHIPS, CS, COLS, SIZE), jnp.bfloat16),
            pltpu.VMEM((CHIPS, ROWS, SIZE), jnp.bfloat16),
            pltpu.SMEM((STRETCHES,), jnp.int32),
            pltpu.VMEM((CHIPS, ROWS + 1, SIZE), jnp.float32),
            pltpu.VMEM((CHIPS, ROWS + 1, SIZE), jnp.float32),
            dma, dma((ZS,)), dma, dma, dma, dma, dma, dma, dma((ZS,)), dma((ZS,)), dma((2,)),
            pltpu.SemaphoreType.REGULAR, pltpu.SemaphoreType.REGULAR,
        ],
        compiler_params=pltpu.CompilerParams(collective_id=0, has_side_effects=True),
    )(
        query_rows.reshape(ROWS, SIZE),
        past_keys.reshape(CHIPS, CS, COLS, SIZE),
        past_values.reshape(CHIPS, CS, COLS, SIZE),
        used_length,
    )
    return read.reshape(query_rows.shape)


def solution(mesh):
    return jax.shard_map(
        body,
        mesh=mesh,
        in_specs=(
            P("ctx", "heads", None, None),
            P(None, "heads", "ctx", None),
            P(None, "heads", "ctx", None),
            P(),
        ),
        out_specs=P("ctx", "heads", None, None),
        check_vma=False,
    )
```

```python
import jax
import jax.numpy as jnp
from jax import lax
from jax.experimental import pallas as pl
from jax.experimental.pallas import tpu as pltpu
from jax.sharding import PartitionSpec as P

MESH = pl.DeviceIdType.MESH
ZS, XS, CS = 8, 4, 2
STRETCHES = ZS * XS * CS
HEADS, GROUP, STRETCH, SIZE = 4, 2, 64, 128
ROWS, COLS = HEADS * GROUP, HEADS * STRETCH
MASKED = -1e30
CHIPS = ZS * XS
FAR = (4, 5, 3, 6, 2, 7, 1, 0)
ACROSS = (2, 1, 3, 0)
EARLY = 2
NEAREST = [min(range(EARLY), key=lambda e: min((z - e) % ZS, (e - z) % ZS)) for z in range(ZS)]


def kernel(
    query, keys, values, lengths, out, k_buf, v_buf, q_buf, len_buf, part, parts,
    q_send, q_recv, p_send, p_recv, k_own, v_own, k_send, v_send, k_recv, v_recv, in_sem, there, all_there,
):
    me = lax.axis_index("ctx")
    my_z, my_x, my_c = me // (XS * CS), lax.rem(me // CS, XS), lax.rem(me, CS)
    chip, beside = me // CS, me + 1 - 2 * my_c
    first = my_z < EARLY

    def turn(k):
        return jnp.where(k < ZS // 2, k, ZS + ZS // 2 - 1 - k)

    def device(z, x):
        return (z * XS + x) * CS + my_c

    def in_plane(z, do):
        for across in ACROSS:
            x = lax.rem(my_x + across, XS)
            if across:
                do(device(z, x))
            else:
                pl.when(z != my_z)(lambda: do(device(z, x)))

    def beyond(do):
        for step in FAR:
            z = lax.rem(my_z + step, ZS)
            pl.when(z >= EARLY)(lambda: in_plane(z, do))

    def within(do):
        for z in range(EARLY):
            in_plane(z, do)

    barrier = pltpu.get_barrier_semaphore()

    def tell(sem, b):
        pl.semaphore_signal(sem, inc=1, device_id={"ctx": b}, device_id_type=MESH)

    def greet(b):
        tell(barrier, b)

    greet(beside)

    @pl.when(first)
    def _():
        beyond(greet)
        within(greet)

    own_copy = pltpu.make_async_copy(query, q_buf.at[chip], in_sem.at[0])
    own_copy.start()
    len_copy = pltpu.make_async_copy(lengths, len_buf, in_sem.at[1])
    len_copy.start()
    k_copy = pltpu.make_async_copy(keys.at[:, my_c], k_buf.at[:, my_c], k_own)
    k_copy.start()
    v_copy = pltpu.make_async_copy(values.at[:, my_c], v_buf.at[:, my_c], v_own)
    v_copy.start()
    pl.when(first)(lambda: pl.semaphore_wait(barrier, EARLY * XS))

    @pl.when(~first)
    def _():
        pl.semaphore_wait(barrier, EARLY * XS + 1)
        within(lambda b: tell(there, b))

    own_copy.wait()
    len_copy.wait()

    def ask(b):
        pltpu.make_async_remote_copy(
            src_ref=q_buf.at[chip],
            dst_ref=q_buf.at[chip],
            send_sem=q_send,
            recv_sem=q_recv.at[my_z],
            device_id={"ctx": b},
            device_id_type=MESH,
        ).start()

    within(ask)

    def swap(z, source, buffer, send_sem, recv_sem):
        rows = pl.ds(z * XS, XS)
        return pltpu.make_async_remote_copy(
            src_ref=source.at[rows, 1 - my_c],
            dst_ref=buffer.at[rows, my_c],
            send_sem=send_sem,
            recv_sem=recv_sem.at[z],
            device_id={"ctx": beside},
            device_id_type=MESH,
        )

    @pl.loop(0, ZS)
    def _(k):
        swap(turn(k), keys, k_buf, k_send, k_recv).start()
        swap(turn(k), values, v_buf, v_send, v_recv).start()

    def arrived(z):
        def wait(n):
            pltpu.make_async_copy(q_buf.at[pl.ds(0, n)], q_buf.at[pl.ds(0, n)], q_recv.at[z]).wait()

        pl.when(z == my_z)(lambda: wait(XS - 1))
        pl.when(z != my_z)(lambda: wait(XS))

    @pl.when(first)
    def _():
        pl.semaphore_wait(there, (ZS - EARLY) * XS)
        for z in range(EARLY, ZS):
            pl.when(my_z == NEAREST[z])(lambda z=z: tell(all_there, device(z, my_x)))

    pl.when(~first)(lambda: pl.semaphore_wait(all_there, 1))
    beyond(ask)
    k_copy.wait()
    v_copy.wait()

    row = lax.broadcasted_iota(jnp.int32, (ROWS, COLS), 0)
    col = lax.broadcasted_iota(jnp.int32, (ROWS, COLS), 1)
    own_head = row // GROUP == col // STRETCH
    position = [(chip * CS + c) * STRETCH + lax.rem(col, STRETCH) for c in range(CS)]
    slot_row = lax.broadcasted_iota(jnp.int32, (ROWS, SIZE), 0)
    slot = lax.broadcasted_iota(jnp.int32, (ROWS, SIZE), 1)

    def answer(z):
        owners = [z * XS + x for x in range(XS)]
        logits = [
            [
                lax.dot_general(q_buf[i], k_buf[i, c], (((1,), (1,)), ((), ())), preferred_element_type=jnp.float32)
                for c in range(CS)
            ]
            for i in owners
        ]
        halves, tops, weights = [], [], []
        for i, pair in zip(owners, logits):
            length = len_buf[i * CS + my_c]
            filled = [own_head & (position[c] < length) for c in range(CS)]
            pair = [jnp.where(f, logit * SIZE ** (-0.5), MASKED) for f, logit in zip(filled, pair)]
            top = jnp.max(jnp.maximum(*pair), axis=1, keepdims=True)
            shares = [jnp.where(f, jnp.exp(logit - top), 0.0) for f, logit in zip(filled, pair)]
            coarse = [share.astype(jnp.bfloat16).astype(jnp.float32) for share in shares]
            halves.append(
                [jnp.concatenate([c, share - c], axis=0).astype(jnp.bfloat16) for c, share in zip(coarse, shares)]
            )
            tops.append(top)
            weights.append(jnp.sum(shares[0] + shares[1], axis=1, keepdims=True))
        reads = [
            sum(jnp.dot(halves_of[c], v_buf[i, c], preferred_element_type=jnp.float32) for c in range(CS))
            for i, halves_of in zip(owners, halves)
        ]
        for i, read, top, weight in zip(owners, reads, tops, weights):
            stats = jnp.where(slot == slot_row, top, jnp.where(slot == slot_row + ROWS, weight, 0.0))
            part[i, pl.ds(0, ROWS), :] = read[:ROWS] + read[ROWS:]
            part[i, pl.ds(ROWS, 1), :] = jnp.sum(stats, axis=0, keepdims=True)

    def give(b):
        pltpu.make_async_remote_copy(
            src_ref=part.at[b // CS],
            dst_ref=parts.at[chip],
            send_sem=p_send,
            recv_sem=p_recv,
            device_id={"ctx": b},
            device_id_type=MESH,
        ).start()

    @pl.loop(0, ZS)
    def _(k):
        z = turn(k)
        arrived(z)
        swap(z, keys, k_buf, k_send, k_recv).wait_recv()
        swap(z, values, v_buf, v_send, v_recv).wait_recv()
        answer(z)
        in_plane(z, give)

    parts[chip] = part[chip]

    rest = pl.ds(0, CHIPS - 1)
    pltpu.make_async_copy(parts.at[rest], parts.at[rest], p_recv).wait()

    stats = parts[:, ROWS, :]
    scale = jnp.exp(stats - jnp.max(stats, axis=0, keepdims=True))
    weight = jnp.sum(scale * pltpu.roll(stats, SIZE - ROWS, 1), axis=0, keepdims=True)
    scale = jnp.transpose(scale / weight)[:ROWS, :]
    total = jnp.zeros((ROWS, SIZE), jnp.float32)
    for s in range(CHIPS):
        total += scale[:, s : s + 1] * parts[s, pl.ds(0, ROWS), :]
    out[...] = total.astype(out.dtype)

    pltpu.make_async_copy(q_buf.at[rest], q_buf.at[rest], q_send).wait()
    pltpu.make_async_copy(part.at[rest], part.at[rest], p_send).wait()
    pltpu.make_async_copy(k_buf.at[:, 0], k_buf.at[:, 0], k_send).wait()
    pltpu.make_async_copy(v_buf.at[:, 0], v_buf.at[:, 0], v_send).wait()


def body(query_rows, past_keys, past_values, used_length):
    anywhere = pl.BlockSpec(memory_space=pl.ANY)
    dma = pltpu.SemaphoreType.DMA
    read = pl.pallas_call(
        kernel,
        out_shape=pltpu.VMEM((ROWS, SIZE), jnp.bfloat16),
        in_specs=[anywhere] * 4,
        out_specs=pl.BlockSpec(memory_space=pltpu.VMEM),
        scratch_shapes=[
            pltpu.VMEM((CHIPS, CS, COLS, SIZE), jnp.bfloat16),
            pltpu.VMEM((CHIPS, CS, COLS, SIZE), jnp.bfloat16),
            pltpu.VMEM((CHIPS, ROWS, SIZE), jnp.bfloat16),
            pltpu.SMEM((STRETCHES,), jnp.int32),
            pltpu.VMEM((CHIPS, ROWS + 1, SIZE), jnp.float32),
            pltpu.VMEM((CHIPS, ROWS + 1, SIZE), jnp.float32),
            dma, dma((ZS,)), dma, dma, dma, dma, dma, dma, dma((ZS,)), dma((ZS,)), dma((2,)),
            pltpu.SemaphoreType.REGULAR, pltpu.SemaphoreType.REGULAR,
        ],
        compiler_params=pltpu.CompilerParams(collective_id=0, has_side_effects=True),
    )(
        query_rows.reshape(ROWS, SIZE),
        past_keys.reshape(CHIPS, CS, COLS, SIZE),
        past_values.reshape(CHIPS, CS, COLS, SIZE),
        used_length,
    )
    return read.reshape(query_rows.shape)


def solution(mesh):
    return jax.shard_map(
        body,
        mesh=mesh,
        in_specs=(
            P("ctx", "heads", None, None),
            P(None, "heads", "ctx", None),
            P(None, "heads", "ctx", None),
            P(),
        ),
        out_specs=P("ctx", "heads", None, None),
        check_vma=False,
    )
```

```python
import jax
import jax.numpy as jnp
from jax import lax
from jax.experimental import pallas as pl
from jax.experimental.pallas import tpu as pltpu
from jax.sharding import PartitionSpec as P

MESH = pl.DeviceIdType.MESH
ZS, XS, CS = 8, 4, 2
STRETCHES = ZS * XS * CS
HEADS, GROUP, STRETCH, SIZE = 4, 2, 64, 128
ROWS, COLS = HEADS * GROUP, HEADS * STRETCH
MASKED = -1e30
CHIPS = ZS * XS
FAR = (4, 5, 3, 6, 2, 7, 1, 0)
ACROSS = (2, 1, 3, 0)
SOON = ZS // 2


def kernel(
    query, keys, values, lengths, out, k_buf, v_buf, q_buf, len_buf, part, parts,
    q_send, q_recv, p_send, p_recv, k_own, v_own, k_send, v_send, k_recv, v_recv, in_sem, there, column, x_there, x_all,
):
    me = lax.axis_index("ctx")
    my_z, my_x, my_c = me // (XS * CS), lax.rem(me // CS, XS), lax.rem(me, CS)
    chip, beside = me // CS, me + 1 - 2 * my_c
    soon = my_z < SOON

    def turn(k):
        return jnp.where(k < ZS // 2, k, ZS + ZS // 2 - 1 - k)

    def device(z, x):
        return (z * XS + x) * CS + my_c

    def in_plane(z, do):
        for across in ACROSS:
            x = lax.rem(my_x + across, XS)
            if across:
                do(device(z, x))
            else:
                pl.when(z != my_z)(lambda: do(device(z, x)))

    def in_column(planes, do):
        for z in planes:
            pl.when(z != my_z)(lambda z=z: do(device(z, my_x)))

    def beside_x(do):
        for across in ACROSS[:-1]:
            do(device(my_z, lax.rem(my_x + across, XS)))

    barrier = pltpu.get_barrier_semaphore()

    def tell(sem, b):
        pl.semaphore_signal(sem, inc=1, device_id={"ctx": b}, device_id_type=MESH)

    def greet(b):
        tell(barrier, b)

    greet(beside)

    pl.when(soon | (my_x == 0))(lambda: beside_x(greet))

    @pl.when(my_z == 0)
    def _():
        for z in range(SOON, ZS):
            in_plane(z, greet)
        in_column(range(1, SOON), greet)

    pl.when(my_z == 1)(lambda: in_column(range(2, ZS), greet))

    own_copy = pltpu.make_async_copy(query, q_buf.at[chip], in_sem.at[0])
    own_copy.start()
    len_copy = pltpu.make_async_copy(lengths, len_buf, in_sem.at[1])
    len_copy.start()
    k_copy = pltpu.make_async_copy(keys.at[:, my_c], k_buf.at[:, my_c], k_own)
    k_copy.start()
    v_copy = pltpu.make_async_copy(values.at[:, my_c], v_buf.at[:, my_c], v_own)
    v_copy.start()
    pl.when(my_z == 0)(lambda: pl.semaphore_wait(barrier, XS))
    pl.when(my_z == 1)(lambda: pl.semaphore_wait(barrier, XS + 1))
    pl.when((my_z >= 2) & (soon | (my_x == 0)))(lambda: pl.semaphore_wait(barrier, XS + 2))
    pl.when(~soon & (my_x != 0))(lambda: pl.semaphore_wait(barrier, XS + 3))
    pl.when(my_z >= 1)(lambda: tell(there, device(0, my_x)))
    pl.when(my_z >= 2)(lambda: tell(there, device(1, my_x)))
    pl.when(~soon & (my_x != 0))(lambda: tell(x_there, device(my_z, 0)))

    own_copy.wait()
    len_copy.wait()

    def ask(b):
        pltpu.make_async_remote_copy(
            src_ref=q_buf.at[chip],
            dst_ref=q_buf.at[chip],
            send_sem=q_send,
            recv_sem=q_recv.at[my_z],
            device_id={"ctx": b},
            device_id_type=MESH,
        ).start()

    pl.when(soon)(lambda: beside_x(ask))
    pl.when(~soon)(lambda: in_plane(0, ask))

    def swap(z, source, buffer, send_sem, recv_sem):
        rows = pl.ds(z * XS, XS)
        return pltpu.make_async_remote_copy(
            src_ref=source.at[rows, 1 - my_c],
            dst_ref=buffer.at[rows, my_c],
            send_sem=send_sem,
            recv_sem=recv_sem.at[z],
            device_id={"ctx": beside},
            device_id_type=MESH,
        )

    @pl.loop(0, ZS)
    def _(k):
        swap(turn(k), keys, k_buf, k_send, k_recv).start()
        swap(turn(k), values, v_buf, v_send, v_recv).start()

    def arrived(z):
        def wait(n):
            pltpu.make_async_copy(q_buf.at[pl.ds(0, n)], q_buf.at[pl.ds(0, n)], q_recv.at[z]).wait()

        pl.when(z == my_z)(lambda: wait(XS - 1))
        pl.when(z != my_z)(lambda: wait(XS))

    def bundle(b):
        rows = pl.ds(my_z * XS, XS)
        pltpu.make_async_remote_copy(
            src_ref=q_buf.at[rows],
            dst_ref=q_buf.at[rows],
            send_sem=q_send,
            recv_sem=q_recv.at[my_z],
            device_id={"ctx": b},
            device_id_type=MESH,
        ).start()

    @pl.when(~soon)
    def _():
        @pl.when(my_x == 0)
        def _():
            pl.semaphore_wait(x_there, XS - 1)
            beside_x(lambda b: tell(x_all, b))

        pl.when(my_x != 0)(lambda: pl.semaphore_wait(x_all, 1))
        beside_x(ask)

    arrived(my_z)

    @pl.when(my_z == 0)
    def _():
        pl.semaphore_wait(there, ZS - 1)
        in_column(range(SOON, ZS), lambda b: tell(column, b))

    @pl.when(my_z == 1)
    def _():
        pl.semaphore_wait(there, ZS - 2)
        in_column(range(2, SOON), lambda b: tell(column, b))

    pl.when(my_z >= 2)(lambda: pl.semaphore_wait(column, 1))
    for step in FAR[:-1]:
        z = lax.rem(my_z + step, ZS)
        pl.when(soon | (z != 0))(lambda z=z: bundle(device(z, my_x)))

    k_copy.wait()
    v_copy.wait()

    row = lax.broadcasted_iota(jnp.int32, (ROWS, COLS), 0)
    col = lax.broadcasted_iota(jnp.int32, (ROWS, COLS), 1)
    own_head = row // GROUP == col // STRETCH
    position = [(chip * CS + c) * STRETCH + lax.rem(col, STRETCH) for c in range(CS)]
    slot_row = lax.broadcasted_iota(jnp.int32, (ROWS, SIZE), 0)
    slot = lax.broadcasted_iota(jnp.int32, (ROWS, SIZE), 1)

    def answer(z):
        owners = [z * XS + x for x in range(XS)]
        logits = [
            [
                lax.dot_general(q_buf[i], k_buf[i, c], (((1,), (1,)), ((), ())), preferred_element_type=jnp.float32)
                for c in range(CS)
            ]
            for i in owners
        ]
        halves, tops, weights = [], [], []
        for i, pair in zip(owners, logits):
            length = len_buf[i * CS + my_c]
            filled = [own_head & (position[c] < length) for c in range(CS)]
            pair = [jnp.where(f, logit * SIZE ** (-0.5), MASKED) for f, logit in zip(filled, pair)]
            top = jnp.max(jnp.maximum(*pair), axis=1, keepdims=True)
            shares = [jnp.where(f, jnp.exp(logit - top), 0.0) for f, logit in zip(filled, pair)]
            coarse = [share.astype(jnp.bfloat16).astype(jnp.float32) for share in shares]
            halves.append(
                [jnp.concatenate([c, share - c], axis=0).astype(jnp.bfloat16) for c, share in zip(coarse, shares)]
            )
            tops.append(top)
            weights.append(jnp.sum(shares[0] + shares[1], axis=1, keepdims=True))
        reads = [
            sum(jnp.dot(halves_of[c], v_buf[i, c], preferred_element_type=jnp.float32) for c in range(CS))
            for i, halves_of in zip(owners, halves)
        ]
        for i, read, top, weight in zip(owners, reads, tops, weights):
            stats = jnp.where(slot == slot_row, top, jnp.where(slot == slot_row + ROWS, weight, 0.0))
            part[i, pl.ds(0, ROWS), :] = read[:ROWS] + read[ROWS:]
            part[i, pl.ds(ROWS, 1), :] = jnp.sum(stats, axis=0, keepdims=True)

    def give(b):
        pltpu.make_async_remote_copy(
            src_ref=part.at[b // CS],
            dst_ref=parts.at[chip],
            send_sem=p_send,
            recv_sem=p_recv,
            device_id={"ctx": b},
            device_id_type=MESH,
        ).start()

    @pl.loop(0, ZS)
    def _(k):
        z = turn(k)
        pl.when(z != my_z)(lambda: arrived(z))
        swap(z, keys, k_buf, k_send, k_recv).wait_recv()
        swap(z, values, v_buf, v_send, v_recv).wait_recv()
        answer(z)
        in_plane(z, give)

    parts[chip] = part[chip]

    rest = pl.ds(0, CHIPS - 1)
    pltpu.make_async_copy(parts.at[rest], parts.at[rest], p_recv).wait()

    stats = parts[:, ROWS, :]
    scale = jnp.exp(stats - jnp.max(stats, axis=0, keepdims=True))
    weight = jnp.sum(scale * pltpu.roll(stats, SIZE - ROWS, 1), axis=0, keepdims=True)
    scale = jnp.transpose(scale / weight)[:ROWS, :]
    total = jnp.zeros((ROWS, SIZE), jnp.float32)
    for s in range(CHIPS):
        total += scale[:, s : s + 1] * parts[s, pl.ds(0, ROWS), :]
    out[...] = total.astype(out.dtype)

    pltpu.make_async_copy(q_buf.at[rest], q_buf.at[rest], q_send).wait()
    pltpu.make_async_copy(part.at[rest], part.at[rest], p_send).wait()
    pltpu.make_async_copy(k_buf.at[:, 0], k_buf.at[:, 0], k_send).wait()
    pltpu.make_async_copy(v_buf.at[:, 0], v_buf.at[:, 0], v_send).wait()


def body(query_rows, past_keys, past_values, used_length):
    anywhere = pl.BlockSpec(memory_space=pl.ANY)
    dma = pltpu.SemaphoreType.DMA
    read = pl.pallas_call(
        kernel,
        out_shape=pltpu.VMEM((ROWS, SIZE), jnp.bfloat16),
        in_specs=[anywhere] * 4,
        out_specs=pl.BlockSpec(memory_space=pltpu.VMEM),
        scratch_shapes=[
            pltpu.VMEM((CHIPS, CS, COLS, SIZE), jnp.bfloat16),
            pltpu.VMEM((CHIPS, CS, COLS, SIZE), jnp.bfloat16),
            pltpu.VMEM((CHIPS, ROWS, SIZE), jnp.bfloat16),
            pltpu.SMEM((STRETCHES,), jnp.int32),
            pltpu.VMEM((CHIPS, ROWS + 1, SIZE), jnp.float32),
            pltpu.VMEM((CHIPS, ROWS + 1, SIZE), jnp.float32),
            dma, dma((ZS,)), dma, dma, dma, dma, dma, dma, dma((ZS,)), dma((ZS,)), dma((2,)),
            *[pltpu.SemaphoreType.REGULAR] * 4,
        ],
        compiler_params=pltpu.CompilerParams(collective_id=0, has_side_effects=True),
    )(
        query_rows.reshape(ROWS, SIZE),
        past_keys.reshape(CHIPS, CS, COLS, SIZE),
        past_values.reshape(CHIPS, CS, COLS, SIZE),
        used_length,
    )
    return read.reshape(query_rows.shape)


def solution(mesh):
    return jax.shard_map(
        body,
        mesh=mesh,
        in_specs=(
            P("ctx", "heads", None, None),
            P(None, "heads", "ctx", None),
            P(None, "heads", "ctx", None),
            P(),
        ),
        out_specs=P("ctx", "heads", None, None),
        check_vma=False,
    )
```

```python
import jax
import jax.numpy as jnp
from jax import lax
from jax.experimental import pallas as pl
from jax.experimental.pallas import tpu as pltpu
from jax.sharding import PartitionSpec as P

MESH = pl.DeviceIdType.MESH
ZS, XS, CS = 8, 4, 2
STRETCHES = ZS * XS * CS
HEADS, GROUP, STRETCH, SIZE = 4, 2, 64, 128
ROWS, COLS = HEADS * GROUP, HEADS * STRETCH
MASKED = -1e30
CHIPS = ZS * XS
FAR = (4, 5, 3, 6, 2, 7, 1, 0)
ACROSS = (2, 1, 3, 0)
SOON = ZS // 2

ORDERS = (
    (0, 1, 2, 3, 4, 5, 6, 7),
    (0, 1, 2, 3, 5, 4, 6, 7),
    (0, 1, 2, 3, 6, 5, 7, 4),
    (0, 1, 2, 3, 7, 6, 5, 4),
    (0, 1, 2, 3, 4, 5, 6, 7),
    (0, 1, 2, 3, 5, 6, 4, 7),
    (0, 1, 2, 3, 6, 5, 7, 4),
    (0, 1, 2, 3, 7, 6, 5, 4),
)

def kernel(
    query, keys, values, lengths, out, k_buf, v_buf, q_buf, len_buf, part, parts,
    q_send, q_recv, p_send, p_recv, k_own, v_own, k_send, v_send, k_recv, v_recv, in_sem, there, column, x_there, x_all, late_recv,
):
    me = lax.axis_index("ctx")
    my_z, my_x, my_c = me // (XS * CS), lax.rem(me // CS, XS), lax.rem(me, CS)
    chip, beside = me // CS, me + 1 - 2 * my_c
    soon = my_z < SOON

    def in_order(do):
        order = 0
        for z, planes in enumerate(ORDERS):
            order = jnp.where(my_z == z, sum(p * ZS**k for k, p in enumerate(planes)), order)

        def step(k, order):
            do(k, lax.rem(order, ZS))
            return order // ZS

        lax.fori_loop(0, ZS, step, order)

    def device(z, x):
        return (z * XS + x) * CS + my_c

    hub = (my_z * XS) * CS + 1

    def spokes(do):
        for x in range(1, XS):
            for c in range(CS):
                do((my_z * XS + x) * CS + c)

    def in_plane(z, do):
        for across in ACROSS:
            x = lax.rem(my_x + across, XS)
            if across:
                do(device(z, x))
            else:
                pl.when(z != my_z)(lambda: do(device(z, x)))

    def in_column(planes, do):
        for z in planes:
            pl.when(z != my_z)(lambda z=z: do(device(z, my_x)))

    def beside_x(do):
        for across in ACROSS[:-1]:
            do(device(my_z, lax.rem(my_x + across, XS)))

    barrier = pltpu.get_barrier_semaphore()

    def tell(sem, b):
        pl.semaphore_signal(sem, inc=1, device_id={"ctx": b}, device_id_type=MESH)

    def greet(b):
        tell(barrier, b)

    greet(beside)

    pl.when(soon)(lambda: beside_x(greet))
    pl.when(~soon & (me == hub))(lambda: spokes(greet))

    @pl.when(my_z == 0)
    def _():
        for z in range(SOON, ZS):
            in_plane(z, greet)
        in_column(range(1, SOON), greet)

    pl.when(my_z == 1)(lambda: in_column(range(2, ZS), greet))

    own_copy = pltpu.make_async_copy(query, q_buf.at[chip], in_sem.at[0])
    own_copy.start()
    len_copy = pltpu.make_async_copy(lengths, len_buf, in_sem.at[1])
    len_copy.start()
    k_copy = pltpu.make_async_copy(keys.at[:, my_c], k_buf.at[:, my_c], k_own)
    k_copy.start()
    v_copy = pltpu.make_async_copy(values.at[:, my_c], v_buf.at[:, my_c], v_own)
    v_copy.start()
    pl.when(my_z == 0)(lambda: pl.semaphore_wait(barrier, XS))
    pl.when(my_z == 1)(lambda: pl.semaphore_wait(barrier, XS + 1))
    pl.when((my_z >= 2) & (soon | (my_x == 0)))(lambda: pl.semaphore_wait(barrier, XS + 2))
    pl.when(~soon & (my_x != 0))(lambda: pl.semaphore_wait(barrier, XS + 3))
    pl.when(my_z >= 1)(lambda: tell(there, device(0, my_x)))
    pl.when(my_z >= 2)(lambda: tell(there, device(1, my_x)))
    pl.when(~soon & (my_x != 0))(lambda: tell(x_there, hub))

    own_copy.wait()
    len_copy.wait()

    def ask(b):
        pltpu.make_async_remote_copy(
            src_ref=q_buf.at[chip],
            dst_ref=q_buf.at[chip],
            send_sem=q_send,
            recv_sem=q_recv.at[my_z],
            device_id={"ctx": b},
            device_id_type=MESH,
        ).start()

    pl.when(soon)(lambda: beside_x(ask))
    pl.when(~soon)(lambda: in_plane(0, ask))

    def swap(z, source, buffer, send_sem, recv_sem):
        rows = pl.ds(z * XS, XS)
        return pltpu.make_async_remote_copy(
            src_ref=source.at[rows, 1 - my_c],
            dst_ref=buffer.at[rows, my_c],
            send_sem=send_sem,
            recv_sem=recv_sem.at[z],
            device_id={"ctx": beside},
            device_id_type=MESH,
        )

    def hand_over(k, z):
        swap(z, keys, k_buf, k_send, k_recv).start()
        swap(z, values, v_buf, v_send, v_recv).start()

    in_order(hand_over)

    def arrived(z):
        def wait(n):
            pltpu.make_async_copy(q_buf.at[pl.ds(0, n)], q_buf.at[pl.ds(0, n)], q_recv.at[z]).wait()

        pl.when(z == my_z)(lambda: wait(XS - 1))
        pl.when(z != my_z)(lambda: wait(XS))

    def bundle(b):
        rows = pl.ds(my_z * XS, XS)
        pltpu.make_async_remote_copy(
            src_ref=q_buf.at[rows],
            dst_ref=q_buf.at[rows],
            send_sem=q_send,
            recv_sem=q_recv.at[my_z],
            device_id={"ctx": b},
            device_id_type=MESH,
        ).start()

    @pl.when(~soon)
    def _():
        @pl.when(me == hub)
        def _():
            pl.semaphore_wait(x_there, (XS - 1) * CS)
            spokes(lambda b: tell(x_all, b))
            tell(x_all, beside)

        pl.when(me != hub)(lambda: pl.semaphore_wait(x_all, 1))
        beside_x(ask)

    arrived(my_z)

    @pl.when(my_z == 0)
    def _():
        pl.semaphore_wait(there, ZS - 1)
        in_column(range(SOON, ZS), lambda b: tell(column, b))

    @pl.when(my_z == 1)
    def _():
        pl.semaphore_wait(there, ZS - 2)
        in_column(range(2, SOON), lambda b: tell(column, b))

    pl.when(my_z >= 2)(lambda: pl.semaphore_wait(column, 1))
    for step in FAR[:-1]:
        z = lax.rem(my_z + step, ZS)
        pl.when(soon | (z >= SOON))(lambda z=z: bundle(device(z, my_x)))

    late = pl.ds(SOON * XS, SOON * XS)

    @pl.when(my_z == 0)
    def _():
        for z in range(SOON, ZS):
            arrived(z)
        for z in range(SOON - 1, 0, -1):
            pltpu.make_async_remote_copy(
                src_ref=q_buf.at[late],
                dst_ref=q_buf.at[late],
                send_sem=q_send,
                recv_sem=late_recv,
                device_id={"ctx": device(z, my_x)},
                device_id_type=MESH,
            ).start()

    k_copy.wait()
    v_copy.wait()

    row = lax.broadcasted_iota(jnp.int32, (ROWS, COLS), 0)
    col = lax.broadcasted_iota(jnp.int32, (ROWS, COLS), 1)
    own_head = row // GROUP == col // STRETCH
    position = [(chip * CS + c) * STRETCH + lax.rem(col, STRETCH) for c in range(CS)]
    slot_row = lax.broadcasted_iota(jnp.int32, (ROWS, SIZE), 0)
    slot = lax.broadcasted_iota(jnp.int32, (ROWS, SIZE), 1)

    def answer(z):
        owners = [z * XS + x for x in range(XS)]
        logits = [
            [
                lax.dot_general(q_buf[i], k_buf[i, c], (((1,), (1,)), ((), ())), preferred_element_type=jnp.float32)
                for c in range(CS)
            ]
            for i in owners
        ]
        halves, tops, weights = [], [], []
        for i, pair in zip(owners, logits):
            length = len_buf[i * CS + my_c]
            filled = [own_head & (position[c] < length) for c in range(CS)]
            pair = [jnp.where(f, logit * SIZE ** (-0.5), MASKED) for f, logit in zip(filled, pair)]
            top = jnp.max(jnp.maximum(*pair), axis=1, keepdims=True)
            shares = [jnp.where(f, jnp.exp(logit - top), 0.0) for f, logit in zip(filled, pair)]
            coarse = [share.astype(jnp.bfloat16).astype(jnp.float32) for share in shares]
            halves.append(
                [jnp.concatenate([c, share - c], axis=0).astype(jnp.bfloat16) for c, share in zip(coarse, shares)]
            )
            tops.append(top)
            weights.append(jnp.sum(shares[0] + shares[1], axis=1, keepdims=True))
        reads = [
            sum(jnp.dot(halves_of[c], v_buf[i, c], preferred_element_type=jnp.float32) for c in range(CS))
            for i, halves_of in zip(owners, halves)
        ]
        for i, read, top, weight in zip(owners, reads, tops, weights):
            stats = jnp.where(slot == slot_row, top, jnp.where(slot == slot_row + ROWS, weight, 0.0))
            part[i, pl.ds(0, ROWS), :] = read[:ROWS] + read[ROWS:]
            part[i, pl.ds(ROWS, 1), :] = jnp.sum(stats, axis=0, keepdims=True)

    def give(b):
        pltpu.make_async_remote_copy(
            src_ref=part.at[b // CS],
            dst_ref=parts.at[chip],
            send_sem=p_send,
            recv_sem=p_recv,
            device_id={"ctx": b},
            device_id_type=MESH,
        ).start()

    def serve(k, z):
        pl.when((z != my_z) & ((z < SOON) | ~soon))(lambda: arrived(z))
        pl.when((k == SOON) & soon & (my_z != 0))(
            lambda: pltpu.make_async_copy(q_buf.at[late], q_buf.at[late], late_recv).wait()
        )
        swap(z, keys, k_buf, k_send, k_recv).wait_recv()
        swap(z, values, v_buf, v_send, v_recv).wait_recv()
        answer(z)
        in_plane(z, give)

    in_order(serve)

    parts[chip] = part[chip]

    rest = pl.ds(0, CHIPS - 1)
    pltpu.make_async_copy(parts.at[rest], parts.at[rest], p_recv).wait()

    stats = parts[:, ROWS, :]
    scale = jnp.exp(stats - jnp.max(stats, axis=0, keepdims=True))
    weight = jnp.sum(scale * pltpu.roll(stats, SIZE - ROWS, 1), axis=0, keepdims=True)
    scale = jnp.transpose(scale / weight)[:ROWS, :]
    total = jnp.zeros((ROWS, SIZE), jnp.float32)
    for s in range(CHIPS):
        total += scale[:, s : s + 1] * parts[s, pl.ds(0, ROWS), :]
    out[...] = total.astype(out.dtype)

    def left(n):
        return lambda: pltpu.make_async_copy(q_buf.at[pl.ds(0, n)], q_buf.at[pl.ds(0, n)], q_send).wait()

    pl.when(soon)(left(XS - 1 + (ZS - 1) * XS))
    pl.when(~soon)(left(XS - 1 + XS + (SOON - 1) * XS))
    for _ in range(1, SOON):
        pl.when(my_z == 0)(left(SOON * XS))
    pltpu.make_async_copy(part.at[rest], part.at[rest], p_send).wait()
    pltpu.make_async_copy(k_buf.at[:, 0], k_buf.at[:, 0], k_send).wait()
    pltpu.make_async_copy(v_buf.at[:, 0], v_buf.at[:, 0], v_send).wait()


def body(query_rows, past_keys, past_values, used_length):
    anywhere = pl.BlockSpec(memory_space=pl.ANY)
    dma = pltpu.SemaphoreType.DMA
    read = pl.pallas_call(
        kernel,
        out_shape=pltpu.VMEM((ROWS, SIZE), jnp.bfloat16),
        in_specs=[anywhere] * 4,
        out_specs=pl.BlockSpec(memory_space=pltpu.VMEM),
        scratch_shapes=[
            pltpu.VMEM((CHIPS, CS, COLS, SIZE), jnp.bfloat16),
            pltpu.VMEM((CHIPS, CS, COLS, SIZE), jnp.bfloat16),
            pltpu.VMEM((CHIPS, ROWS, SIZE), jnp.bfloat16),
            pltpu.SMEM((STRETCHES,), jnp.int32),
            pltpu.VMEM((CHIPS, ROWS + 1, SIZE), jnp.float32),
            pltpu.VMEM((CHIPS, ROWS + 1, SIZE), jnp.float32),
            dma, dma((ZS,)), dma, dma, dma, dma, dma, dma, dma((ZS,)), dma((ZS,)), dma((2,)),
            *[pltpu.SemaphoreType.REGULAR] * 4, dma,
        ],
        compiler_params=pltpu.CompilerParams(collective_id=0, has_side_effects=True),
    )(
        query_rows.reshape(ROWS, SIZE),
        past_keys.reshape(CHIPS, CS, COLS, SIZE),
        past_values.reshape(CHIPS, CS, COLS, SIZE),
        used_length,
    )
    return read.reshape(query_rows.shape)


def solution(mesh):
    return jax.shard_map(
        body,
        mesh=mesh,
        in_specs=(
            P("ctx", "heads", None, None),
            P(None, "heads", "ctx", None),
            P(None, "heads", "ctx", None),
            P(),
        ),
        out_specs=P("ctx", "heads", None, None),
        check_vma=False,
    )
```
